32 devices in a mesh: dp: 8 (over z, y), group: 4 (over x, core).
Axes of the slice: x: 2, y: 2, z: 4, core: 2. Of those that a mesh axis runs over, the one named last changes fastest.
Arguments:
- rewards: bfloat16 [8192, 4096], P(('dp', 'group')), may hold values from -6 to 6
- values: bfloat16 [8192, 4096], P(('dp', 'group')), may hold values from -6 to 6
- lengths: int32 [8192], P(('dp', 'group')), may hold values from 1 to 4096
- decay_rate: float32 [8192], P(('dp', 'group')), may hold values from 3.8146973e-06 to 0.03125
- piece_dest: int32 [8, 8], P('dp'), may hold values from 0 to 7, each once within a row
- row_perm: int32 [64, 128], P(('dp', 'group')), may hold values from 0 to 127, each once within a row
- minibatch: int32 [8192], P(('dp', 'group')), may hold values from 0 to 63
Outputs:
- white_rewards: bfloat16 [8192, 4096], P(('dp', 'group'))
- white_advantage: bfloat16 [8192, 4096], P(('dp', 'group'))
The draws below stay inside these ranges and needn't reach their ends.
Inputs may be any that keep to these rules, and one draw needn't show every extreme that they name: Each row of piece_dest names every index of dp once. Each row of row_perm names every number below 128 once.
All inputs are finite; a program needn't handle non-finite values.
Results may differ from the reference program's by a relative error of at most 0.0049.
Values may be sent and summed in bfloat16 or wider, within the bound.
A program may use at most 64 MiB of HBM per device.

```python
import math
import jax
import jax.numpy as jnp
from jax import lax

LEN = 4096
BLK = 128
ROWS_DEV = 256
MINIBATCHES = 64
ROWS = 8192
BLOCKS = 64
N_DP = 8
N_GROUP = 4


def plant(result, rng, least, high):
    shape = result.shape
    index_at = [jax.random.randint(jax.random.fold_in(rng, axis), (), 0, shape[axis]) for axis in range(len(shape))]
    result = result.at[tuple(index_at)].set(least)
    longest = shape.index(max(shape))
    index_at[longest] = (index_at[longest] + 1) % shape[longest]
    return result.at[tuple(index_at)].set(high)


def shard_levels(rng, dims, pieces, least, high):
    gain, own = 1.0, jax.random.fold_in(rng, 6)
    for dim, blocks in pieces:
        heights = jnp.exp(jax.random.uniform(jax.random.fold_in(own, dim), (blocks,), jnp.float32, least / len(pieces), high / len(pieces)))
        gain = gain * jnp.repeat(heights, dims[dim] // blocks).reshape([-1 if axis == dim else 1 for axis in range(len(dims))])
    return gain


def centred(key, extent, scale, most, pieces=(), kind=jnp.bfloat16):
    entries = scale * jax.random.normal(key, extent, jnp.float32)
    if pieces:
        entries = entries * shard_levels(key, extent, pieces, -0.22, 0.18)
    return jnp.clip(entries, -most, most).astype(kind)


def setup_inputs(seed: int = 0) -> dict:
    streams_of = jax.random.split(jax.random.key(seed), 8)
    return {
        "rewards": centred(streams_of[0], (ROWS, LEN), 1.0, 6.0, ((0, 32),)),
        "values": centred(streams_of[1], (ROWS, LEN), 1.0, 6.0, ((0, 32),)),
        "lengths": plant(jax.random.randint(streams_of[2], (ROWS,), 1, LEN + 1), jax.random.fold_in(streams_of[2], 1), 1, LEN).astype(jnp.int32),
        "decay_rate": jnp.clip(jnp.exp(math.log(0.03125) - 9.010913 * jax.random.uniform(streams_of[3], (ROWS,), jnp.float32) ** shard_levels(streams_of[3], (ROWS,), ((0, 32),), -0.2, 0.2)), 3.814697265625e-06, 0.03125),
        "piece_dest": jax.vmap(lambda own: jax.random.permutation(own, N_DP))(jax.random.split(streams_of[4], N_DP)).reshape((N_DP, N_DP)).astype(jnp.int32),
        "row_perm": jax.vmap(lambda own: jax.random.permutation(own, BLK))(jax.random.split(streams_of[5], BLOCKS)).reshape((BLOCKS, BLK)).astype(jnp.int32),
        "minibatch": plant(jax.random.randint(streams_of[6], (ROWS,), 0, MINIBATCHES), jax.random.fold_in(streams_of[6], 1), 0, MINIBATCHES - 1).astype(jnp.int32),
    }


def reference(rewards, values, lengths, decay_rate, piece_dest, row_perm, minibatch):
    rows_all, span_all = rewards.shape
    position = jnp.arange(span_all, dtype=jnp.int32)
    is_valid = position[None, :] < lengths[:, None]
    next_valid = position[None, :] + 1 < lengths[:, None]
    per_step = jnp.exp(-decay_rate)
    value_f = values.astype(jnp.float32)
    value_next = jnp.concatenate([value_f[:, 1:], jnp.zeros((rows_all, 1), jnp.float32)], axis=1)
    td_error = rewards.astype(jnp.float32) + per_step[:, None] * jnp.where(next_valid, value_next, 0.0) - value_f
    td_error = jnp.where(is_valid, td_error, 0.0)

    def backward(carry, column):
        fresh = column + per_step * carry
        return (fresh, fresh)
    starting = jnp.zeros((rows_all,), jnp.float32)
    final_carry, stacked = lax.scan(backward, starting, td_error.T, reverse=True)
    advantage = stacked.T.astype(jnp.bfloat16)
    piece = ROWS_DEV // N_DP
    source_slot = jnp.argsort(piece_dest, axis=1).astype(jnp.int32)
    out_rows = jnp.arange(rows_all, dtype=jnp.int32)
    device = out_rows // ROWS_DEV
    target = device // N_GROUP
    column_group = device % N_GROUP
    inside = out_rows % ROWS_DEV
    chosen = inside // BLK * BLK + row_perm.reshape(-1).astype(jnp.int32)
    source_dev = chosen // piece
    within = chosen % piece
    source_row = (source_dev * N_GROUP + column_group) * ROWS_DEV + source_slot[source_dev, target] * piece + within
    moved_rewards = jnp.take(rewards, source_row, axis=0).astype(jnp.float32)
    moved_advantage = jnp.take(advantage, source_row, axis=0).astype(jnp.float32)
    moved_lengths = jnp.take(lengths, source_row, axis=0)
    valid = position[None, :] < moved_lengths[:, None]
    moved_rewards = jnp.where(valid, moved_rewards, 0.0)
    moved_advantage = jnp.where(valid, moved_advantage, 0.0)
    count = jax.ops.segment_sum(moved_lengths.astype(jnp.float32), minibatch, num_segments=MINIBATCHES)
    count = jnp.maximum(count, 1.0)

    def whiten(moved):
        mean = jax.ops.segment_sum(lax.optimization_barrier(jnp.sum(moved, axis=1)), minibatch, num_segments=MINIBATCHES) / count
        deviation = jnp.where(valid, moved - mean[minibatch][:, None], 0.0)
        spread = jax.ops.segment_sum(lax.optimization_barrier(jnp.sum(deviation * deviation, axis=1)), minibatch, num_segments=MINIBATCHES) / count
        return (deviation / jnp.sqrt(spread[minibatch][:, None] + 1e-05)).astype(jnp.bfloat16)
    return (whiten(moved_rewards), whiten(moved_advantage))
```

```python
import functools

import jax
import jax.numpy as jnp
from jax import lax
from jax.experimental import pallas as pl
from jax.experimental.pallas import tpu as pltpu
from jax.sharding import PartitionSpec as P

MINIBATCHES = 64


HIGHEST = lax.Precision.HIGHEST


def discounted(rewards, values, lengths, decay_rate):
    rows_here, span = rewards.shape
    block = min(128, span)
    blocks_here = span // block
    position = jnp.arange(span, dtype=jnp.int32)
    is_valid = position[None, :] < lengths[:, None]
    next_valid = position[None, :] + 1 < lengths[:, None]
    per_step = jnp.exp(-decay_rate)
    value_f = values.astype(jnp.float32)
    value_next = jnp.concatenate([value_f[:, 1:], jnp.zeros((rows_here, 1), jnp.float32)], axis=1)
    td_error = (
        rewards.astype(jnp.float32)
        + per_step[:, None] * jnp.where(next_valid, value_next, 0.0)
        - value_f
    )
    td_error = jnp.where(is_valid, td_error, 0.0).reshape(rows_here, blocks_here, block)
    offset = jnp.arange(block, dtype=jnp.float32)
    lower_scale = jnp.exp(-decay_rate[:, None] * offset[None, :])
    upper_scale = jnp.exp(decay_rate[:, None] * offset[None, :])
    triangle = (offset[:, None] >= offset[None, :]).astype(jnp.float32)
    scaled = td_error * lower_scale[:, None, :]
    summed = jnp.einsum("rjk,kt->rjt", scaled, triangle, precision=HIGHEST)
    local_part = summed * upper_scale[:, None, :]
    heads = local_part[:, :, 0]
    block_step = jnp.exp(-decay_rate * block)

    def carry_step(carry, head):
        fresh = head + block_step * carry
        return (fresh, fresh)

    final_carry, starts = lax.scan(carry_step, jnp.zeros_like(decay_rate), heads.T, reverse=True)
    next_heads = jnp.concatenate([starts[1:].T, jnp.zeros((rows_here, 1), jnp.float32)], axis=1)
    reach = jnp.exp(-decay_rate[:, None] * (block - offset[None, :]))
    total = local_part + reach[:, None, :] * next_heads[:, :, None]
    return jnp.where(is_valid, total.reshape(rows_here, span), 0.0).astype(jnp.bfloat16)


def by_target(array, piece_dest):
    peers = piece_dest.shape[1]
    target = piece_dest[0]
    slots = jnp.arange(peers, dtype=jnp.int32)
    source_slot = jnp.sum(jnp.where(target[None, :] == slots[:, None], slots[None, :], 0), axis=1)
    pieces = array.reshape((peers, array.shape[0] // peers) + array.shape[1:])
    return jnp.take(pieces, source_slot, axis=0).reshape(array.shape)


def reorder(received, row_perm):
    blocks_here, block = row_perm.shape
    chooser = (row_perm[:, :, None] == jnp.arange(block, dtype=jnp.int32)[None, None, :]).astype(
        jnp.bfloat16
    )

    def permute_one(member):
        shaped = member.reshape(blocks_here, block, member.shape[-1])
        mixed = jnp.einsum("bim,bmc->bic", chooser, shaped, preferred_element_type=jnp.float32)
        return mixed.astype(jnp.bfloat16).reshape(member.shape)

    return tuple((permute_one(member) for member in received))


def whiten(rewards, advantage, lengths, minibatch):
    rows_here, span = rewards.shape
    position = jnp.arange(span, dtype=jnp.int32)
    is_valid = position[None, :] < lengths[:, None]
    counted = lengths.astype(jnp.float32)
    reward_f = jnp.where(is_valid, rewards.astype(jnp.float32), 0.0)
    advantage_f = jnp.where(is_valid, advantage.astype(jnp.float32), 0.0)
    member = (minibatch[:, None] == jnp.arange(MINIBATCHES, dtype=jnp.int32)[None, :]).astype(
        jnp.float32
    )
    row_terms = jnp.stack(
        [
            counted,
            jnp.sum(reward_f, axis=1),
            jnp.sum(advantage_f, axis=1),
            jnp.sum(reward_f * reward_f, axis=1),
            jnp.sum(advantage_f * advantage_f, axis=1),
        ],
        axis=1,
    )
    totals = lax.psum(jnp.dot(member.T, row_terms, precision=HIGHEST), ("dp", "group"))
    count = jnp.maximum(totals[:, 0], 1.0)
    means = totals[:, 1:3] / count[:, None]
    spreads = totals[:, 3:5] / count[:, None] - means * means
    row_means = jnp.dot(member, means, precision=HIGHEST)
    row_scale = jnp.dot(member, lax.rsqrt(spreads + 1e-05), precision=HIGHEST)
    white_rewards = jnp.where(is_valid, (reward_f - row_means[:, 0:1]) * row_scale[:, 0:1], 0.0)
    white_advantage = jnp.where(
        is_valid, (advantage_f - row_means[:, 1:2]) * row_scale[:, 1:2], 0.0
    )
    return (white_rewards.astype(jnp.bfloat16), white_advantage.astype(jnp.bfloat16))


def plain_local(rewards, values, lengths, decay_rate, piece_dest, row_perm, minibatch):
    blocks_here, block = row_perm.shape
    new_order = (jnp.arange(blocks_here, dtype=jnp.int32)[:, None] * block + row_perm).reshape(-1)
    per_row = jnp.stack([lengths.astype(jnp.float32), decay_rate], axis=1)
    moved_terms = lax.all_to_all(
        by_target(per_row, piece_dest), "dp", split_axis=0, concat_axis=0, tiled=True
    )
    moved_terms = jnp.take(moved_terms, new_order, axis=0)
    lengths_here = moved_terms[:, 0].astype(jnp.int32)
    rate_here = moved_terms[:, 1]
    moved_rewards, moved_second = reorder(
        (
            lax.all_to_all(
                by_target(rewards, piece_dest), "dp", split_axis=0, concat_axis=0, tiled=True
            ),
            lax.all_to_all(
                by_target(values, piece_dest), "dp", split_axis=0, concat_axis=0, tiled=True
            ),
        ),
        row_perm,
    )
    advantage = discounted(moved_rewards, moved_second, lengths_here, rate_here)
    return whiten(moved_rewards, advantage, lengths_here, minibatch)


F32 = jnp.float32
BF16 = jnp.bfloat16
LANES = 128
MESH = pl.DeviceIdType.MESH
NT = (((1,), (1,)), ((), ()))


def exchange_kernel(
    n_dp, n_group,
    rew_hbm, val_hbm, lens_ref, rate_ref, dest_ref, perm_ref, mb_ref,
    out_r, out_a, out_st, out_ch,
    rbuf, vbuf, abuf, rsend, asend, tri, lower, upper, lenb, bstep, carry,
    acc, tbuf, tstage, tsend, trecv, psend, precv, qsend, qrecv, tot,
    load_sem, own_sem, rs_sem, rr_sem, as_sem, ar_sem, ts_sem, tr_sem, ps_sem, pr_sem, qs_sem, qr_sem,
):
    rows, span = rew_hbm.shape
    blocks = perm_ref.shape[0]
    piece = rows // n_dp
    wide = tri.shape[0]
    halves = as_sem.shape[0]
    half = span // halves
    me = lax.axis_index("dp")
    mine = lax.axis_index("group")
    order = sorted(range(1, n_dp), key=lambda d: (abs(2 * d - n_dp), d))

    def dp_peer(d):
        return lax.rem(me + d, n_dp)

    def group_peer(d):
        return lax.rem(mine + d, n_group)

    quarter = rows // 4
    loads = []
    for which, (src, dst) in enumerate(((rew_hbm, rbuf), (val_hbm, vbuf))):
        for part in range(4):
            at = pl.ds(part * quarter, quarter)
            loads.append(
                pltpu.make_async_copy(src.at[at], dst.at[at], load_sem.at[4 * which + part])
            )
            loads[-1].start()

    barrier = pltpu.get_barrier_semaphore()
    for d in range(1, n_dp):
        pl.semaphore_signal(barrier, inc=1, device_id=(dp_peer(d), mine), device_id_type=MESH)
    for d in range(1, n_group):
        pl.semaphore_signal(barrier, inc=1, device_id=(me, group_peer(d)), device_id_type=MESH)

    def pick(d, source, columns):
        k = dp_peer(d)
        width = 512 if columns == span else columns
        weights = [
            (jnp.full((piece, width), dest_ref[0, p], jnp.int32) == k).astype(F32).astype(source.dtype)
            for p in range(n_dp)
        ]
        for c in range(0, columns, width):
            at = slice(c, c + width)
            yield at, sum(source[p * piece : (p + 1) * piece, at] * weights[p] for p in range(n_dp))

    for load in loads[:4]:
        load.wait()

    def stage(d, source, target):
        for at, part in pick(d, source, span):
            target[d, :, at] = part

    stage(order[0], rbuf, rsend)
    pl.semaphore_wait(barrier, n_dp + n_group - 2)

    def remote(src, dst, send, recv, who):
        return pltpu.make_async_remote_copy(
            src_ref=src, dst_ref=dst, send_sem=send, recv_sem=recv,
            device_id=who, device_id_type=MESH,
        )

    sent = []
    for d, later in zip(order, order[1:] + [0]):
        stage(later, rbuf, rsend)
        k = dp_peer(d)
        sent.append(remote(rsend.at[d], out_r.at[me], rs_sem.at[d], rr_sem.at[d], (k, mine)))
        sent[-1].start()
    own = [pltpu.make_async_copy(rsend.at[0], out_r.at[me], own_sem.at[0])]
    own[0].start()

    for b in range(blocks):
        at = pl.ds(b * LANES, LANES)
        rate = jnp.transpose(jnp.broadcast_to(rate_ref[b : b + 1, :], (LANES, LANES)))
        length = jnp.transpose(
            jnp.broadcast_to(lens_ref[b : b + 1, :].astype(F32), (LANES, LANES))
        )
        lenb[at, :] = length.astype(jnp.int32)
        bstep[at, :] = jnp.exp(-rate * wide)
        carry[at, :] = jnp.zeros((LANES, LANES), F32)
        for x in range(4):
            acc[x, at, :] = jnp.zeros((LANES, LANES), F32)
        for h in range(wide // LANES):
            offset = (lax.broadcasted_iota(jnp.int32, (LANES, LANES), 1) + h * LANES).astype(F32)
            lower[at, h * LANES : (h + 1) * LANES] = jnp.exp(-rate * offset)
            upper[at, h * LANES : (h + 1) * LANES] = jnp.exp(rate * offset)
    tri[...] = (
        lax.broadcasted_iota(jnp.int32, (wide, wide), 0)
        >= lax.broadcasted_iota(jnp.int32, (wide, wide), 1)
    ).astype(F32).astype(BF16)
    for load in loads[4:]:
        load.wait()

    reps = wide // LANES

    def column_step(i, _):
        col = pl.multiple_of((span // wide - 1 - i) * wide, wide)
        for b in range(blocks):
            at = pl.ds(b * LANES, LANES)
            length = lenb[at, :]
            position = col + lax.broadcasted_iota(jnp.int32, (LANES, wide), 1)
            valid = position < jnp.concatenate([length] * reps, axis=1)
            r = jnp.where(valid, rbuf[at, pl.ds(col, wide)].astype(F32), 0.0)
            s = r * lower[at, :]
            high = s.astype(BF16)
            low = (s - high.astype(F32)).astype(BF16)
            both = jnp.dot(
                jnp.concatenate([high, low], axis=0), tri[...], preferred_element_type=F32
            )
            c = carry[at, :]
            summed = both[:LANES] + both[LANES:] + jnp.concatenate([c] * reps, axis=1)
            carry[at, :] = bstep[at, :] * jnp.broadcast_to(summed[:, :1], (LANES, LANES))
            a = upper[at, :] * summed - vbuf[at, pl.ds(col, wide)].astype(F32)
            a = jnp.where(valid, a, 0.0).astype(BF16)
            abuf[at, pl.ds(col, wide)] = a
            a = a.astype(F32)
            for x, term in enumerate((r, a, r * r, a * a)):
                acc[x, at, :] += sum(term[:, h * LANES : (h + 1) * LANES] for h in range(reps))
        return 0

    lax.fori_loop(0, span // wide, column_step, 0)

    lane = lax.broadcasted_iota(jnp.int32, (LANES, LANES), 1)
    for b in range(blocks):
        at = pl.ds(b * LANES, LANES)
        terms = jnp.where(lane == 0, lenb[at, :].astype(F32), 0.0)
        for x in range(4):
            total = jnp.sum(acc[x, at, :], axis=1, keepdims=True)
            terms = jnp.where(lane == x + 1, total, terms)
        tbuf[at, :] = terms
    tstage[...] = jnp.zeros_like(tstage)

    def stage_second(d, _):
        stage(d, abuf, asend)
        for at, part in pick(d, tbuf, LANES):
            tstage[0:piece, :] = part
        tsend[d] = jnp.transpose(tstage[...])[0:8, :]
        return 0

    lax.fori_loop(0, n_dp, stage_second, 0)

    terms_sent = []
    for d in order:
        k = dp_peer(d)
        terms_sent.append(remote(tsend.at[d], trecv.at[me], ts_sem.at[d], tr_sem.at[d], (k, mine)))
        terms_sent[-1].start()
    trecv[me] = tsend[0]

    def send_second(part):
        at = pl.ds(part * half, half)
        for d in order:
            k = dp_peer(d)
            sent.append(
                remote(
                    asend.at[d, :, at], out_a.at[me, :, at],
                    as_sem.at[part, d], ar_sem.at[part, d], (k, mine),
                )
            )
            sent[-1].start()

    send_second(0)
    own.append(pltpu.make_async_copy(asend.at[0], out_a.at[me], own_sem.at[1]))
    own[1].start()

    for copy in terms_sent:
        copy.wait()

    row = lax.broadcasted_iota(jnp.int32, (LANES, LANES), 0)
    partial = jnp.zeros((8, LANES), F32)
    per_block = LANES // piece
    for b in range(blocks):
        picked = (row == perm_ref[b : b + 1, :]).astype(F32)
        member = (row == mb_ref[b : b + 1, :]).astype(F32)
        arrived_member = lax.dot_general(
            member.astype(BF16), picked.astype(BF16), NT, preferred_element_type=F32
        )
        terms = trecv[b * per_block]
        for s in range(1, per_block):
            terms = terms + pltpu.roll(trecv[b * per_block + s], s * piece, 1)
        partial = partial + lax.dot_general(
            terms, arrived_member, NT, precision=HIGHEST, preferred_element_type=F32
        )
        out_ch[b] = jnp.transpose(picked).astype(BF16)
        tot[b] = jnp.dot(terms, picked, precision=HIGHEST, preferred_element_type=F32)
    psend[...] = partial
    precv[me] = partial
    sums_sent = []
    for d in order:
        k = dp_peer(d)
        sums_sent.append(remote(psend, precv.at[me], ps_sem.at[d], pr_sem.at[d], (k, mine)))
        sums_sent[-1].start()

    for part in range(1, halves):
        send_second(part)

    for copy in sums_sent:
        copy.wait()
    partial = precv[0]
    for k in range(1, n_dp):
        partial = partial + precv[k]
    qsend[...] = partial
    qrecv[mine] = partial
    group_sent = []
    for d in range(1, n_group):
        k = group_peer(d)
        group_sent.append(remote(qsend, qrecv.at[mine], qs_sem.at[d], qr_sem.at[d], (me, k)))
        group_sent[-1].start()
    for copy in group_sent:
        copy.wait()
    total = qrecv[0]
    for k in range(1, n_group):
        total = total + qrecv[k]

    count = jnp.maximum(total[0:1, :], 1.0)
    means = total[1:3, :] / count
    spreads = jnp.maximum(total[3:5, :] / count - means * means, 0.0)
    scales = lax.rsqrt(spreads + 1e-05)
    table = jnp.concatenate([means, scales, jnp.zeros((4, LANES), F32)], axis=0)
    for b in range(blocks):
        at = pl.ds(b * LANES, LANES)
        member = (row == mb_ref[b : b + 1, :]).astype(F32)
        here = jnp.dot(table, member, precision=HIGHEST, preferred_element_type=F32)
        here = jnp.concatenate(
            [here[0:4, :], tot[b, 0:1, :], jnp.zeros((LANES - 5, LANES), F32)], axis=0
        )
        out_st[at, :] = jnp.transpose(here)

    for copy in own + sent:
        copy.wait()


def exchange(n_dp, n_group, rewards, values, lengths, decay_rate, piece_dest, row_perm, minibatch):
    rows, span = rewards.shape
    blocks, block = row_perm.shape
    piece = rows // n_dp
    wide = 256
    vmem = pl.BlockSpec(memory_space=pltpu.VMEM)
    far = pl.BlockSpec(memory_space=pltpu.HBM)
    dma = pltpu.SemaphoreType.DMA
    whole = pltpu.VMEM((rows, span), BF16)
    staged = pltpu.VMEM((n_dp, piece, span), BF16)
    factor = pltpu.VMEM((rows, wide), F32)
    column = pltpu.VMEM((rows, LANES), F32)
    small = pltpu.VMEM((n_dp, 8, LANES), F32)
    one = pltpu.VMEM((8, LANES), F32)
    return pl.pallas_call(
        functools.partial(exchange_kernel, n_dp, n_group),
        out_shape=(
            jax.ShapeDtypeStruct((n_dp, piece, span), BF16),
            jax.ShapeDtypeStruct((n_dp, piece, span), BF16),
            jax.ShapeDtypeStruct((rows, LANES), F32),
            jax.ShapeDtypeStruct((blocks, LANES, LANES), BF16),
        ),
        in_specs=[
            far, far, vmem, vmem, pl.BlockSpec(memory_space=pltpu.SMEM), vmem, vmem,
        ],
        out_specs=(vmem, vmem, vmem, vmem),
        scratch_shapes=[
            whole, whole, whole, staged, staged,
            pltpu.VMEM((wide, wide), BF16), factor, factor,
            pltpu.VMEM((rows, LANES), jnp.int32), column, column,
            pltpu.VMEM((4, rows, LANES), F32), column, pltpu.VMEM((LANES, LANES), F32),
            small, small, one, small, one, pltpu.VMEM((n_group, 8, LANES), F32),
            pltpu.VMEM((blocks, 8, LANES), F32),
            dma((8,)), dma((2,)), dma((n_dp,)), dma((n_dp,)), dma((2, n_dp)), dma((2, n_dp)),
            dma((n_dp,)), dma((n_dp,)), dma((n_dp,)), dma((n_dp,)), dma((n_group,)), dma((n_group,)),
        ],
        compiler_params=pltpu.CompilerParams(
            collective_id=0, has_side_effects=True, vmem_limit_bytes=40 * 1024 * 1024
        ),
    )(
        rewards, values, lengths.reshape(blocks, block), decay_rate.reshape(blocks, block),
        piece_dest, row_perm, minibatch.reshape(blocks, block),
    )


def whiten_kernel(blocks, r_ref, a_ref, st_ref, ch_ref, wr_ref, wa_ref):
    tile = wr_ref.shape[1]
    first = pl.multiple_of(pl.program_id(0) * tile, tile)
    for b in range(blocks):
        at = pl.ds(b * LANES, LANES)
        stats = st_ref[at, :]
        position = (first + lax.broadcasted_iota(jnp.int32, (LANES, tile), 1)).astype(F32)
        valid = position < stats[:, 4:5]
        for x, (src, dst) in enumerate(((r_ref, wr_ref), (a_ref, wa_ref))):
            moved = jnp.dot(ch_ref[b], src[at, pl.ds(first, tile)], preferred_element_type=F32)
            white = (moved - stats[:, x : x + 1]) * stats[:, x + 2 : x + 3]
            dst[at, :] = jnp.where(valid, white, 0.0).astype(BF16)


def whiten_moved(rewards, advantage, stats, chooser):
    rows, span = rewards.shape
    blocks = chooser.shape[0]
    tile = min(512, span)
    data = pl.BlockSpec((rows, tile), lambda i: (0, i))
    return pl.pallas_call(
        functools.partial(whiten_kernel, blocks),
        grid=(span // tile,),
        out_shape=(jax.ShapeDtypeStruct((rows, span), BF16),) * 2,
        in_specs=[pl.BlockSpec(memory_space=pltpu.VMEM)] * 4,
        out_specs=(data, data),
    )(rewards, advantage, stats, chooser)


def local(n_dp, n_group, rewards, values, lengths, decay_rate, piece_dest, row_perm, minibatch):
    rows, span = rewards.shape
    if (rows // n_dp) % 16 or LANES % (rows // n_dp) or row_perm.shape[1] != LANES or span % 1024:
        return plain_local(rewards, values, lengths, decay_rate, piece_dest, row_perm, minibatch)
    moved_r, moved_a, stats, chooser = exchange(
        n_dp, n_group, rewards, values, lengths, decay_rate, piece_dest, row_perm, minibatch
    )
    return whiten_moved(
        moved_r.reshape(rows, span), moved_a.reshape(rows, span), stats, chooser
    )


def solution(mesh):
    return jax.shard_map(
        functools.partial(local, mesh.shape["dp"], mesh.shape["group"]),
        mesh=mesh,
        in_specs=(
            P(("dp", "group"), None),
            P(("dp", "group"), None),
            P(("dp", "group")),
            P(("dp", "group")),
            P("dp", None),
            P(("dp", "group"), None),
            P(("dp", "group")),
        ),
        out_specs=(P(("dp", "group"), None), P(("dp", "group"), None)),
        check_vma=False,
    )
```

```python
import functools

import jax
import jax.numpy as jnp
from jax import lax
from jax.experimental import pallas as pl
from jax.experimental.pallas import tpu as pltpu
from jax.sharding import PartitionSpec as P

MINIBATCHES = 64


HIGHEST = lax.Precision.HIGHEST


def discounted(rewards, values, lengths, decay_rate):
    rows_here, span = rewards.shape
    block = min(128, span)
    blocks_here = span // block
    position = jnp.arange(span, dtype=jnp.int32)
    is_valid = position[None, :] < lengths[:, None]
    next_valid = position[None, :] + 1 < lengths[:, None]
    per_step = jnp.exp(-decay_rate)
    value_f = values.astype(jnp.float32)
    value_next = jnp.concatenate([value_f[:, 1:], jnp.zeros((rows_here, 1), jnp.float32)], axis=1)
    td_error = (
        rewards.astype(jnp.float32)
        + per_step[:, None] * jnp.where(next_valid, value_next, 0.0)
        - value_f
    )
    td_error = jnp.where(is_valid, td_error, 0.0).reshape(rows_here, blocks_here, block)
    offset = jnp.arange(block, dtype=jnp.float32)
    lower_scale = jnp.exp(-decay_rate[:, None] * offset[None, :])
    upper_scale = jnp.exp(decay_rate[:, None] * offset[None, :])
    triangle = (offset[:, None] >= offset[None, :]).astype(jnp.float32)
    scaled = td_error * lower_scale[:, None, :]
    summed = jnp.einsum("rjk,kt->rjt", scaled, triangle, precision=HIGHEST)
    local_part = summed * upper_scale[:, None, :]
    heads = local_part[:, :, 0]
    block_step = jnp.exp(-decay_rate * block)

    def carry_step(carry, head):
        fresh = head + block_step * carry
        return (fresh, fresh)

    final_carry, starts = lax.scan(carry_step, jnp.zeros_like(decay_rate), heads.T, reverse=True)
    next_heads = jnp.concatenate([starts[1:].T, jnp.zeros((rows_here, 1), jnp.float32)], axis=1)
    reach = jnp.exp(-decay_rate[:, None] * (block - offset[None, :]))
    total = local_part + reach[:, None, :] * next_heads[:, :, None]
    return jnp.where(is_valid, total.reshape(rows_here, span), 0.0).astype(jnp.bfloat16)


def by_target(array, piece_dest):
    peers = piece_dest.shape[1]
    target = piece_dest[0]
    slots = jnp.arange(peers, dtype=jnp.int32)
    source_slot = jnp.sum(jnp.where(target[None, :] == slots[:, None], slots[None, :], 0), axis=1)
    pieces = array.reshape((peers, array.shape[0] // peers) + array.shape[1:])
    return jnp.take(pieces, source_slot, axis=0).reshape(array.shape)


def reorder(received, row_perm):
    blocks_here, block = row_perm.shape
    chooser = (row_perm[:, :, None] == jnp.arange(block, dtype=jnp.int32)[None, None, :]).astype(
        jnp.bfloat16
    )

    def permute_one(member):
        shaped = member.reshape(blocks_here, block, member.shape[-1])
        mixed = jnp.einsum("bim,bmc->bic", chooser, shaped, preferred_element_type=jnp.float32)
        return mixed.astype(jnp.bfloat16).reshape(member.shape)

    return tuple((permute_one(member) for member in received))


def whiten(rewards, advantage, lengths, minibatch):
    rows_here, span = rewards.shape
    position = jnp.arange(span, dtype=jnp.int32)
    is_valid = position[None, :] < lengths[:, None]
    counted = lengths.astype(jnp.float32)
    reward_f = jnp.where(is_valid, rewards.astype(jnp.float32), 0.0)
    advantage_f = jnp.where(is_valid, advantage.astype(jnp.float32), 0.0)
    member = (minibatch[:, None] == jnp.arange(MINIBATCHES, dtype=jnp.int32)[None, :]).astype(
        jnp.float32
    )
    row_terms = jnp.stack(
        [
            counted,
            jnp.sum(reward_f, axis=1),
            jnp.sum(advantage_f, axis=1),
            jnp.sum(reward_f * reward_f, axis=1),
            jnp.sum(advantage_f * advantage_f, axis=1),
        ],
        axis=1,
    )
    totals = lax.psum(jnp.dot(member.T, row_terms, precision=HIGHEST), ("dp", "group"))
    count = jnp.maximum(totals[:, 0], 1.0)
    means = totals[:, 1:3] / count[:, None]
    spreads = totals[:, 3:5] / count[:, None] - means * means
    row_means = jnp.dot(member, means, precision=HIGHEST)
    row_scale = jnp.dot(member, lax.rsqrt(spreads + 1e-05), precision=HIGHEST)
    white_rewards = jnp.where(is_valid, (reward_f - row_means[:, 0:1]) * row_scale[:, 0:1], 0.0)
    white_advantage = jnp.where(
        is_valid, (advantage_f - row_means[:, 1:2]) * row_scale[:, 1:2], 0.0
    )
    return (white_rewards.astype(jnp.bfloat16), white_advantage.astype(jnp.bfloat16))


def plain_local(rewards, values, lengths, decay_rate, piece_dest, row_perm, minibatch):
    blocks_here, block = row_perm.shape
    new_order = (jnp.arange(blocks_here, dtype=jnp.int32)[:, None] * block + row_perm).reshape(-1)
    per_row = jnp.stack([lengths.astype(jnp.float32), decay_rate], axis=1)
    moved_terms = lax.all_to_all(
        by_target(per_row, piece_dest), "dp", split_axis=0, concat_axis=0, tiled=True
    )
    moved_terms = jnp.take(moved_terms, new_order, axis=0)
    lengths_here = moved_terms[:, 0].astype(jnp.int32)
    rate_here = moved_terms[:, 1]
    moved_rewards, moved_second = reorder(
        (
            lax.all_to_all(
                by_target(rewards, piece_dest), "dp", split_axis=0, concat_axis=0, tiled=True
            ),
            lax.all_to_all(
                by_target(values, piece_dest), "dp", split_axis=0, concat_axis=0, tiled=True
            ),
        ),
        row_perm,
    )
    advantage = discounted(moved_rewards, moved_second, lengths_here, rate_here)
    return whiten(moved_rewards, advantage, lengths_here, minibatch)


F32 = jnp.float32
BF16 = jnp.bfloat16
LANES = 128
MESH = pl.DeviceIdType.MESH
NT = (((1,), (1,)), ((), ()))


def exchange_kernel(
    n_dp, n_group,
    rbuf, val_hbm, packed,
    white_r, white_a,
    out_r, out_a, out_st, out_ch,
    vbuf, abuf, rsend, asend, tri, lower, upper, lenb, bstep, carry,
    acc, tbuf, tstage, tsend, trecv, psend, precv, qsend, qrecv, tot,
    load_sem, own_sem, rs_sem, rr_sem, as_sem, ar_sem, ts_sem, tr_sem, ps_sem, pr_sem, qs_sem, qr_sem,
):
    rows, span = rbuf.shape
    blocks = out_ch.shape[0]
    piece = rows // n_dp
    wide = tri.shape[0]
    cuts = ((0, span // 2), (span // 2, span // 4), (3 * span // 4, span // 4))
    me = lax.axis_index("dp")
    mine = lax.axis_index("group")
    order = sorted(range(1, n_dp), key=lambda d: (abs(2 * d - n_dp), d))

    def dp_peer(d):
        return lax.rem(me + d, n_dp)

    def group_peer(d):
        return lax.rem(mine + d, n_group)

    quarter = rows // 4
    loads = []
    for part in range(4):
        at = pl.ds(part * quarter, quarter)
        loads.append(pltpu.make_async_copy(val_hbm.at[at], vbuf.at[at], load_sem.at[part]))
        loads[-1].start()

    def row_of(kind, b):
        return packed[kind * blocks + b : kind * blocks + b + 1, :]

    barrier = pltpu.get_barrier_semaphore()
    for d in range(1, n_dp):
        pl.semaphore_signal(barrier, inc=1, device_id=(dp_peer(d), mine), device_id_type=MESH)
    for d in range(1, n_group):
        pl.semaphore_signal(barrier, inc=1, device_id=(me, group_peer(d)), device_id_type=MESH)

    targets = [
        jnp.broadcast_to(row_of(4, 0)[:, p : p + 1], (piece, LANES)) for p in range(n_dp)
    ]

    def pick(d, source):
        k = jnp.full((piece, LANES), dp_peer(d), jnp.int32).astype(F32)
        weights = [(target == k).astype(F32).astype(source.dtype) for target in targets]
        for c in range(0, source.shape[1], LANES):
            at = slice(c, c + LANES)
            yield at, sum(source[p * piece : (p + 1) * piece, at] * weights[p] for p in range(n_dp))

    def stage(d, source, target):
        for at, part in pick(d, source):
            target[d, :, at] = part

    stage(order[0], rbuf, rsend)
    pl.semaphore_wait(barrier, n_dp + n_group - 2)

    def remote(src, dst, send, recv, who):
        return pltpu.make_async_remote_copy(
            src_ref=src, dst_ref=dst, send_sem=send, recv_sem=recv,
            device_id=who, device_id_type=MESH,
        )

    sent = []
    second = []
    for d, later in zip(order, order[1:] + [0]):
        stage(later, rbuf, rsend)
        k = dp_peer(d)
        sent.append(remote(rsend.at[d], out_r.at[me], rs_sem.at[d], rr_sem.at[d], (k, mine)))
        sent[-1].start()
    own = [pltpu.make_async_copy(rsend.at[0], out_r.at[me], own_sem.at[0])]
    own[0].start()

    for b in range(blocks):
        at = pl.ds(b * LANES, LANES)
        rate = jnp.transpose(jnp.broadcast_to(row_of(1, b), (LANES, LANES)))
        length = jnp.transpose(jnp.broadcast_to(row_of(0, b), (LANES, LANES)))
        lenb[at, :] = length.astype(jnp.int32)
        bstep[at, :] = jnp.exp(-rate * wide)
        carry[at, :] = jnp.zeros((LANES, LANES), F32)
        for x in range(4):
            acc[x, at, :] = jnp.zeros((LANES, LANES), F32)
        for h in range(wide // LANES):
            offset = (lax.broadcasted_iota(jnp.int32, (LANES, LANES), 1) + h * LANES).astype(F32)
            lower[at, h * LANES : (h + 1) * LANES] = jnp.exp(-rate * offset)
            upper[at, h * LANES : (h + 1) * LANES] = jnp.exp(rate * offset)
    tri[...] = (
        lax.broadcasted_iota(jnp.int32, (wide, wide), 0)
        >= lax.broadcasted_iota(jnp.int32, (wide, wide), 1)
    ).astype(F32).astype(BF16)
    for load in loads:
        load.wait()

    reps = wide // LANES

    def column_step(i, _):
        col = pl.multiple_of((span // wide - 1 - i) * wide, wide)
        for b in range(blocks):
            at = pl.ds(b * LANES, LANES)
            length = lenb[at, :]
            position = col + lax.broadcasted_iota(jnp.int32, (LANES, wide), 1)
            valid = position < jnp.concatenate([length] * reps, axis=1)
            r = jnp.where(valid, rbuf[at, pl.ds(col, wide)].astype(F32), 0.0)
            s = r * lower[at, :]
            high = s.astype(BF16)
            low = (s - high.astype(F32)).astype(BF16)
            both = jnp.dot(
                jnp.concatenate([high, low], axis=0), tri[...], preferred_element_type=F32
            )
            c = carry[at, :]
            summed = both[:LANES] + both[LANES:] + jnp.concatenate([c] * reps, axis=1)
            carry[at, :] = bstep[at, :] * jnp.broadcast_to(summed[:, :1], (LANES, LANES))
            a = upper[at, :] * summed - vbuf[at, pl.ds(col, wide)].astype(F32)
            a = jnp.where(valid, a, 0.0).astype(BF16)
            abuf[at, pl.ds(col, wide)] = a
            a = a.astype(F32)
            for x, term in enumerate((r, a, r * r, a * a)):
                acc[x, at, :] += sum(term[:, h * LANES : (h + 1) * LANES] for h in range(reps))
        return 0

    lax.fori_loop(0, span // wide, column_step, 0)

    lane = lax.broadcasted_iota(jnp.int32, (LANES, LANES), 1)
    for b in range(blocks):
        at = pl.ds(b * LANES, LANES)
        terms = jnp.where(lane == 0, lenb[at, :].astype(F32), 0.0)
        for x in range(4):
            total = jnp.sum(acc[x, at, :], axis=1, keepdims=True)
            terms = jnp.where(lane == x + 1, total, terms)
        tbuf[at, :] = terms
    tstage[...] = jnp.zeros_like(tstage)

    def stage_second(d, _):
        stage(d, abuf, asend)
        for at, part in pick(d, tbuf):
            tstage[0:piece, :] = part
        tsend[d] = jnp.transpose(tstage[...])[0:8, :]
        return 0

    lax.fori_loop(0, n_dp, stage_second, 0)

    terms_sent = []
    for d in order:
        k = dp_peer(d)
        terms_sent.append(remote(tsend.at[d], trecv.at[me], ts_sem.at[d], tr_sem.at[d], (k, mine)))
        terms_sent[-1].start()
    trecv[me] = tsend[0]

    def send_second(part):
        at = pl.ds(*cuts[part])
        second.append([])
        for d in order:
            k = dp_peer(d)
            second[part].append(
                remote(
                    asend.at[d, :, at], out_a.at[me, :, at],
                    as_sem.at[part, d], ar_sem.at[part, d], (k, mine),
                )
            )
            second[part][-1].start()

    send_second(0)
    own.append(pltpu.make_async_copy(asend.at[0], out_a.at[me], own_sem.at[1]))
    own[1].start()

    for copy in terms_sent:
        copy.wait()

    row = lax.broadcasted_iota(jnp.int32, (LANES, LANES), 0).astype(F32)
    partial = jnp.zeros((8, LANES), F32)
    per_block = LANES // piece
    for b in range(blocks):
        picked = (row == row_of(2, b)).astype(F32)
        member = (row == row_of(3, b)).astype(F32)
        arrived_member = lax.dot_general(
            member.astype(BF16), picked.astype(BF16), NT, preferred_element_type=F32
        )
        terms = trecv[b * per_block]
        for s in range(1, per_block):
            terms = terms + pltpu.roll(trecv[b * per_block + s], s * piece, 1)
        partial = partial + lax.dot_general(
            terms, arrived_member, NT, precision=HIGHEST, preferred_element_type=F32
        )
        out_ch[b] = jnp.transpose(picked).astype(BF16)
        tot[b] = jnp.dot(terms, picked, precision=HIGHEST, preferred_element_type=F32)
    psend[...] = partial
    precv[me] = partial
    sums_sent = []
    for d in order:
        k = dp_peer(d)
        sums_sent.append(remote(psend, precv.at[me], ps_sem.at[d], pr_sem.at[d], (k, mine)))
        sums_sent[-1].start()

    for part in range(1, len(cuts)):
        send_second(part)

    for copy in sums_sent:
        copy.wait()
    partial = precv[0]
    for k in range(1, n_dp):
        partial = partial + precv[k]
    qsend[...] = partial
    qrecv[mine] = partial
    group_sent = []
    for d in range(1, n_group):
        k = group_peer(d)
        group_sent.append(remote(qsend, qrecv.at[mine], qs_sem.at[d], qr_sem.at[d], (me, k)))
        group_sent[-1].start()
    for copy in group_sent:
        copy.wait()
    total = qrecv[0]
    for k in range(1, n_group):
        total = total + qrecv[k]

    count = jnp.maximum(total[0:1, :], 1.0)
    means = total[1:3, :] / count
    spreads = jnp.maximum(total[3:5, :] / count - means * means, 0.0)
    scales = lax.rsqrt(spreads + 1e-05)
    table = jnp.concatenate([means, scales, jnp.zeros((4, LANES), F32)], axis=0)
    for b in range(blocks):
        at = pl.ds(b * LANES, LANES)
        member = (row == row_of(3, b)).astype(F32)
        here = jnp.dot(table, member, precision=HIGHEST, preferred_element_type=F32)
        here = jnp.concatenate(
            [here[0:4, :], tot[b, 0:1, :], jnp.zeros((LANES - 5, LANES), F32)], axis=0
        )
        out_st[at, :] = jnp.transpose(here)

    def whiten_part(x, source, target, start, width):
        tile = min(512, width)

        def tile_step(i, _):
            col = pl.multiple_of(start + i * tile, tile)
            for b in range(blocks):
                at = pl.ds(b * LANES, LANES)
                stats = out_st[at, :]
                position = (col + lax.broadcasted_iota(jnp.int32, (LANES, tile), 1)).astype(F32)
                arrived = source[b * per_block : (b + 1) * per_block, :, pl.ds(col, tile)]
                moved = jnp.dot(
                    out_ch[b], arrived.reshape(LANES, tile), preferred_element_type=F32
                )
                white = (moved - stats[:, x : x + 1]) * stats[:, x + 2 : x + 3]
                white = jnp.where(position < stats[:, 4:5], white, 0.0)
                target[at, pl.ds(col, tile)] = white.astype(BF16)
            return 0

        lax.fori_loop(0, width // tile, tile_step, 0)

    for copy in own + sent:
        copy.wait()
    whiten_part(0, out_r, white_r, 0, span)
    for part, copies in enumerate(second):
        for copy in copies:
            copy.wait_recv()
        whiten_part(1, out_a, white_a, *cuts[part])
    for copies in second:
        for copy in copies:
            copy.wait_send()


def exchange(n_dp, n_group, rewards, values, lengths, decay_rate, piece_dest, row_perm, minibatch):
    rows, span = rewards.shape
    blocks, block = row_perm.shape
    piece = rows // n_dp
    wide = 256
    vmem = pl.BlockSpec(memory_space=pltpu.VMEM)
    far = pl.BlockSpec(memory_space=pltpu.HBM)
    dma = pltpu.SemaphoreType.DMA
    whole = pltpu.VMEM((rows, span), BF16)
    staged = pltpu.VMEM((n_dp, piece, span), BF16)
    factor = pltpu.VMEM((rows, wide), F32)
    column = pltpu.VMEM((rows, LANES), F32)
    small = pltpu.VMEM((n_dp, 8, LANES), F32)
    one = pltpu.VMEM((8, LANES), F32)
    return pl.pallas_call(
        functools.partial(exchange_kernel, n_dp, n_group),
        out_shape=(jax.ShapeDtypeStruct((rows, span), BF16),) * 2,
        in_specs=[vmem, far, vmem],
        out_specs=(vmem, vmem),
        scratch_shapes=[
            staged, staged, column, pltpu.VMEM((blocks, LANES, LANES), BF16),
            whole, whole, staged, staged,
            pltpu.VMEM((wide, wide), BF16), factor, factor,
            pltpu.VMEM((rows, LANES), jnp.int32), column, column,
            pltpu.VMEM((4, rows, LANES), F32), column, pltpu.VMEM((LANES, LANES), F32),
            small, small, one, small, one, pltpu.VMEM((n_group, 8, LANES), F32),
            pltpu.VMEM((blocks, 8, LANES), F32),
            dma((4,)), dma((2,)), dma((n_dp,)), dma((n_dp,)), dma((3, n_dp)), dma((3, n_dp)),
            dma((n_dp,)), dma((n_dp,)), dma((n_dp,)), dma((n_dp,)), dma((n_group,)), dma((n_group,)),
        ],
        compiler_params=pltpu.CompilerParams(
            collective_id=0, has_side_effects=True, vmem_limit_bytes=50_000_000
        ),
    )(
        rewards, values,
        jnp.concatenate(
            [
                lengths.astype(F32).reshape(blocks, block),
                decay_rate.reshape(blocks, block),
                row_perm.astype(F32),
                minibatch.astype(F32).reshape(blocks, block),
                jnp.pad(piece_dest.astype(F32), ((0, 0), (0, block - piece_dest.shape[1]))),
            ],
            axis=0,
        ),
    )


def local(n_dp, n_group, rewards, values, lengths, decay_rate, piece_dest, row_perm, minibatch):
    rows, span = rewards.shape
    if (rows // n_dp) % 16 or LANES % (rows // n_dp) or row_perm.shape[1] != LANES or span % 1024:
        return plain_local(rewards, values, lengths, decay_rate, piece_dest, row_perm, minibatch)
    return exchange(
        n_dp, n_group, rewards, values, lengths, decay_rate, piece_dest, row_perm, minibatch
    )


def solution(mesh):
    return jax.shard_map(
        functools.partial(local, mesh.shape["dp"], mesh.shape["group"]),
        mesh=mesh,
        in_specs=(
            P(("dp", "group"), None),
            P(("dp", "group"), None),
            P(("dp", "group")),
            P(("dp", "group")),
            P("dp", None),
            P(("dp", "group"), None),
            P(("dp", "group")),
        ),
        out_specs=(P(("dp", "group"), None), P(("dp", "group"), None)),
        check_vma=False,
    )
```

```python
import functools

import jax
import jax.numpy as jnp
from jax import lax
from jax.experimental import pallas as pl
from jax.experimental.pallas import tpu as pltpu
from jax.sharding import PartitionSpec as P

MINIBATCHES = 64


HIGHEST = lax.Precision.HIGHEST


def discounted(rewards, values, lengths, decay_rate):
    rows_here, span = rewards.shape
    block = min(128, span)
    blocks_here = span // block
    position = jnp.arange(span, dtype=jnp.int32)
    is_valid = position[None, :] < lengths[:, None]
    next_valid = position[None, :] + 1 < lengths[:, None]
    per_step = jnp.exp(-decay_rate)
    value_f = values.astype(jnp.float32)
    value_next = jnp.concatenate([value_f[:, 1:], jnp.zeros((rows_here, 1), jnp.float32)], axis=1)
    td_error = (
        rewards.astype(jnp.float32)
        + per_step[:, None] * jnp.where(next_valid, value_next, 0.0)
        - value_f
    )
    td_error = jnp.where(is_valid, td_error, 0.0).reshape(rows_here, blocks_here, block)
    offset = jnp.arange(block, dtype=jnp.float32)
    lower_scale = jnp.exp(-decay_rate[:, None] * offset[None, :])
    upper_scale = jnp.exp(decay_rate[:, None] * offset[None, :])
    triangle = (offset[:, None] >= offset[None, :]).astype(jnp.float32)
    scaled = td_error * lower_scale[:, None, :]
    summed = jnp.einsum("rjk,kt->rjt", scaled, triangle, precision=HIGHEST)
    local_part = summed * upper_scale[:, None, :]
    heads = local_part[:, :, 0]
    block_step = jnp.exp(-decay_rate * block)

    def carry_step(carry, head):
        fresh = head + block_step * carry
        return (fresh, fresh)

    final_carry, starts = lax.scan(carry_step, jnp.zeros_like(decay_rate), heads.T, reverse=True)
    next_heads = jnp.concatenate([starts[1:].T, jnp.zeros((rows_here, 1), jnp.float32)], axis=1)
    reach = jnp.exp(-decay_rate[:, None] * (block - offset[None, :]))
    total = local_part + reach[:, None, :] * next_heads[:, :, None]
    return jnp.where(is_valid, total.reshape(rows_here, span), 0.0).astype(jnp.bfloat16)


def by_target(array, piece_dest):
    peers = piece_dest.shape[1]
    target = piece_dest[0]
    slots = jnp.arange(peers, dtype=jnp.int32)
    source_slot = jnp.sum(jnp.where(target[None, :] == slots[:, None], slots[None, :], 0), axis=1)
    pieces = array.reshape((peers, array.shape[0] // peers) + array.shape[1:])
    return jnp.take(pieces, source_slot, axis=0).reshape(array.shape)


def reorder(received, row_perm):
    blocks_here, block = row_perm.shape
    chooser = (row_perm[:, :, None] == jnp.arange(block, dtype=jnp.int32)[None, None, :]).astype(
        jnp.bfloat16
    )

    def permute_one(member):
        shaped = member.reshape(blocks_here, block, member.shape[-1])
        mixed = jnp.einsum("bim,bmc->bic", chooser, shaped, preferred_element_type=jnp.float32)
        return mixed.astype(jnp.bfloat16).reshape(member.shape)

    return tuple((permute_one(member) for member in received))


def whiten(rewards, advantage, lengths, minibatch):
    rows_here, span = rewards.shape
    position = jnp.arange(span, dtype=jnp.int32)
    is_valid = position[None, :] < lengths[:, None]
    counted = lengths.astype(jnp.float32)
    reward_f = jnp.where(is_valid, rewards.astype(jnp.float32), 0.0)
    advantage_f = jnp.where(is_valid, advantage.astype(jnp.float32), 0.0)
    member = (minibatch[:, None] == jnp.arange(MINIBATCHES, dtype=jnp.int32)[None, :]).astype(
        jnp.float32
    )
    row_terms = jnp.stack(
        [
            counted,
            jnp.sum(reward_f, axis=1),
            jnp.sum(advantage_f, axis=1),
            jnp.sum(reward_f * reward_f, axis=1),
            jnp.sum(advantage_f * advantage_f, axis=1),
        ],
        axis=1,
    )
    totals = lax.psum(jnp.dot(member.T, row_terms, precision=HIGHEST), ("dp", "group"))
    count = jnp.maximum(totals[:, 0], 1.0)
    means = totals[:, 1:3] / count[:, None]
    spreads = totals[:, 3:5] / count[:, None] - means * means
    row_means = jnp.dot(member, means, precision=HIGHEST)
    row_scale = jnp.dot(member, lax.rsqrt(spreads + 1e-05), precision=HIGHEST)
    white_rewards = jnp.where(is_valid, (reward_f - row_means[:, 0:1]) * row_scale[:, 0:1], 0.0)
    white_advantage = jnp.where(
        is_valid, (advantage_f - row_means[:, 1:2]) * row_scale[:, 1:2], 0.0
    )
    return (white_rewards.astype(jnp.bfloat16), white_advantage.astype(jnp.bfloat16))


def plain_local(rewards, values, lengths, decay_rate, piece_dest, row_perm, minibatch):
    blocks_here, block = row_perm.shape
    new_order = (jnp.arange(blocks_here, dtype=jnp.int32)[:, None] * block + row_perm).reshape(-1)
    per_row = jnp.stack([lengths.astype(jnp.float32), decay_rate], axis=1)
    moved_terms = lax.all_to_all(
        by_target(per_row, piece_dest), "dp", split_axis=0, concat_axis=0, tiled=True
    )
    moved_terms = jnp.take(moved_terms, new_order, axis=0)
    lengths_here = moved_terms[:, 0].astype(jnp.int32)
    rate_here = moved_terms[:, 1]
    moved_rewards, moved_second = reorder(
        (
            lax.all_to_all(
                by_target(rewards, piece_dest), "dp", split_axis=0, concat_axis=0, tiled=True
            ),
            lax.all_to_all(
                by_target(values, piece_dest), "dp", split_axis=0, concat_axis=0, tiled=True
            ),
        ),
        row_perm,
    )
    advantage = discounted(moved_rewards, moved_second, lengths_here, rate_here)
    return whiten(moved_rewards, advantage, lengths_here, minibatch)


F32 = jnp.float32
BF16 = jnp.bfloat16
LANES = 128
MESH = pl.DeviceIdType.MESH
NT = (((1,), (1,)), ((), ()))


def exchange_kernel(
    n_dp, n_group,
    rbuf, val_hbm, rate_ref, packed,
    white_r, white_a,
    out_r, out_a, out_st, out_ch,
    vbuf, abuf, rsend, asend, tri, lower, upper, lenb, bstep, carry,
    acc, tbuf, tstage, tsend, trecv, psend, precv, qsend, qrecv, tot,
    load_sem, own_sem, rs_sem, rr_sem, as_sem, ar_sem, ts_sem, tr_sem, ps_sem, pr_sem, qs_sem, qr_sem,
):
    rows, span = rbuf.shape
    blocks = out_ch.shape[0]
    piece = rows // n_dp
    wide = tri.shape[0]
    cuts = ((0, span // 2), (span // 2, 3 * span // 8), (7 * span // 8, span // 8))
    me = lax.axis_index("dp")
    mine = lax.axis_index("group")
    order = sorted(range(1, n_dp), key=lambda d: (abs(2 * d - n_dp), d))

    def dp_peer(d):
        return lax.rem(me + d, n_dp)

    def group_peer(d):
        return lax.rem(mine + d, n_group)

    quarter = rows // 4
    loads = []
    for part in range(4):
        at = pl.ds(part * quarter, quarter)
        loads.append(pltpu.make_async_copy(val_hbm.at[at], vbuf.at[at], load_sem.at[part]))
        loads[-1].start()

    def row_of(kind, b):
        return packed[kind * blocks + b : kind * blocks + b + 1, :].astype(F32)

    barrier = pltpu.get_barrier_semaphore()
    for d in range(1, n_dp):
        pl.semaphore_signal(barrier, inc=1, device_id=(dp_peer(d), mine), device_id_type=MESH)
    for d in range(1, n_group):
        pl.semaphore_signal(barrier, inc=1, device_id=(me, group_peer(d)), device_id_type=MESH)

    targets = [
        jnp.broadcast_to(row_of(3, 0)[:, p : p + 1], (piece, LANES)) for p in range(n_dp)
    ]

    def pick(d, source):
        k = jnp.full((piece, LANES), dp_peer(d), jnp.int32).astype(F32)
        weights = [(target == k).astype(F32).astype(source.dtype) for target in targets]
        for c in range(0, source.shape[1], LANES):
            at = slice(c, c + LANES)
            yield at, sum(source[p * piece : (p + 1) * piece, at] * weights[p] for p in range(n_dp))

    def stage(d, source, target):
        for at, part in pick(d, source):
            target[d, :, at] = part

    stage(order[0], rbuf, rsend)
    pl.semaphore_wait(barrier, n_dp + n_group - 2)

    def remote(src, dst, send, recv, who):
        return pltpu.make_async_remote_copy(
            src_ref=src, dst_ref=dst, send_sem=send, recv_sem=recv,
            device_id=who, device_id_type=MESH,
        )

    sent = []
    second = []
    for d, later in zip(order, order[1:] + [0]):
        stage(later, rbuf, rsend)
        k = dp_peer(d)
        sent.append(remote(rsend.at[d], out_r.at[me], rs_sem.at[d], rr_sem.at[d], (k, mine)))
        sent[-1].start()
    own = [pltpu.make_async_copy(rsend.at[0], out_r.at[me], own_sem.at[0])]
    own[0].start()

    for b in range(blocks):
        at = pl.ds(b * LANES, LANES)
        rate = jnp.transpose(jnp.broadcast_to(rate_ref[b : b + 1, :], (LANES, LANES)))
        length = jnp.transpose(jnp.broadcast_to(row_of(0, b), (LANES, LANES)))
        lenb[at, :] = length.astype(jnp.int32)
        bstep[at, :] = jnp.exp(-rate * wide)
        carry[at, :] = jnp.zeros((LANES, LANES), F32)
        for x in range(4):
            acc[x, at, :] = jnp.zeros((LANES, LANES), F32)
        for h in range(wide // LANES):
            offset = (lax.broadcasted_iota(jnp.int32, (LANES, LANES), 1) + h * LANES).astype(F32)
            lower[at, h * LANES : (h + 1) * LANES] = jnp.exp(-rate * offset)
            upper[at, h * LANES : (h + 1) * LANES] = jnp.exp(rate * offset)
    tri[...] = (
        lax.broadcasted_iota(jnp.int32, (wide, wide), 0)
        >= lax.broadcasted_iota(jnp.int32, (wide, wide), 1)
    ).astype(F32).astype(BF16)
    for load in loads:
        load.wait()

    reps = wide // LANES

    def column_step(i, _):
        col = pl.multiple_of((span // wide - 1 - i) * wide, wide)
        for b in range(blocks):
            at = pl.ds(b * LANES, LANES)
            length = lenb[at, :]
            position = col + lax.broadcasted_iota(jnp.int32, (LANES, wide), 1)
            valid = position < jnp.concatenate([length] * reps, axis=1)
            r = jnp.where(valid, rbuf[at, pl.ds(col, wide)].astype(F32), 0.0)
            s = r * lower[at, :]
            high = s.astype(BF16)
            low = (s - high.astype(F32)).astype(BF16)
            both = jnp.dot(
                jnp.concatenate([high, low], axis=0), tri[...], preferred_element_type=F32
            )
            c = carry[at, :]
            summed = both[:LANES] + both[LANES:] + jnp.concatenate([c] * reps, axis=1)
            carry[at, :] = bstep[at, :] * jnp.broadcast_to(summed[:, :1], (LANES, LANES))
            a = upper[at, :] * summed - vbuf[at, pl.ds(col, wide)].astype(F32)
            a = jnp.where(valid, a, 0.0).astype(BF16)
            abuf[at, pl.ds(col, wide)] = a
            a = a.astype(F32)
            for x, term in enumerate((r, a, r * r, a * a)):
                acc[x, at, :] += sum(term[:, h * LANES : (h + 1) * LANES] for h in range(reps))
        return 0

    lax.fori_loop(0, span // wide, column_step, 0)

    lane = lax.broadcasted_iota(jnp.int32, (LANES, LANES), 1)
    for b in range(blocks):
        at = pl.ds(b * LANES, LANES)
        terms = jnp.where(lane == 0, lenb[at, :].astype(F32), 0.0)
        for x in range(4):
            total = jnp.sum(acc[x, at, :], axis=1, keepdims=True)
            terms = jnp.where(lane == x + 1, total, terms)
        tbuf[at, :] = terms
    tstage[...] = jnp.zeros_like(tstage)

    def stage_second(d, _):
        stage(d, abuf, asend)
        for at, part in pick(d, tbuf):
            tstage[0:piece, :] = part
        tsend[d] = jnp.transpose(tstage[...])[0:8, :]
        return 0

    lax.fori_loop(0, n_dp, stage_second, 0)

    terms_sent = []
    for d in order:
        k = dp_peer(d)
        terms_sent.append(remote(tsend.at[d], trecv.at[me], ts_sem.at[d], tr_sem.at[d], (k, mine)))
        terms_sent[-1].start()
    trecv[me] = tsend[0]

    def send_second(part):
        at = pl.ds(*cuts[part])
        second.append([])
        for d in order:
            k = dp_peer(d)
            second[part].append(
                remote(
                    asend.at[d, :, at], out_a.at[me, :, at],
                    as_sem.at[part, d], ar_sem.at[part, d], (k, mine),
                )
            )
            second[part][-1].start()

    send_second(0)
    own.append(pltpu.make_async_copy(asend.at[0], out_a.at[me], own_sem.at[1]))
    own[1].start()

    for copy in terms_sent:
        copy.wait()

    row = lax.broadcasted_iota(jnp.int32, (LANES, LANES), 0).astype(F32)
    partial = jnp.zeros((8, LANES), F32)
    per_block = LANES // piece
    for b in range(blocks):
        picked = (row == row_of(1, b)).astype(F32)
        member = (row == row_of(2, b)).astype(F32)
        arrived_member = lax.dot_general(
            member.astype(BF16), picked.astype(BF16), NT, preferred_element_type=F32
        )
        terms = trecv[b * per_block]
        for s in range(1, per_block):
            terms = terms + pltpu.roll(trecv[b * per_block + s], s * piece, 1)
        partial = partial + lax.dot_general(
            terms, arrived_member, NT, precision=HIGHEST, preferred_element_type=F32
        )
        out_ch[b] = jnp.transpose(picked).astype(BF16)
        tot[b] = jnp.dot(terms, picked, precision=HIGHEST, preferred_element_type=F32)
    psend[...] = partial
    precv[me] = partial
    sums_sent = []
    for d in order:
        k = dp_peer(d)
        sums_sent.append(remote(psend, precv.at[me], ps_sem.at[d], pr_sem.at[d], (k, mine)))
        sums_sent[-1].start()

    for part in range(1, len(cuts)):
        send_second(part)

    for copy in sums_sent:
        copy.wait()
    partial = precv[0]
    for k in range(1, n_dp):
        partial = partial + precv[k]
    qsend[...] = partial
    qrecv[mine] = partial
    group_sent = []
    for d in range(1, n_group):
        k = group_peer(d)
        group_sent.append(remote(qsend, qrecv.at[mine], qs_sem.at[d], qr_sem.at[d], (me, k)))
        group_sent[-1].start()
    for copy in group_sent:
        copy.wait()
    total = qrecv[0]
    for k in range(1, n_group):
        total = total + qrecv[k]

    count = jnp.maximum(total[0:1, :], 1.0)
    means = total[1:3, :] / count
    spreads = jnp.maximum(total[3:5, :] / count - means * means, 0.0)
    scales = lax.rsqrt(spreads + 1e-05)
    table = jnp.concatenate([means, scales, jnp.zeros((4, LANES), F32)], axis=0)
    for b in range(blocks):
        at = pl.ds(b * LANES, LANES)
        member = (row == row_of(2, b)).astype(F32)
        here = jnp.dot(table, member, precision=HIGHEST, preferred_element_type=F32)
        here = jnp.concatenate(
            [here[0:4, :], tot[b, 0:1, :], jnp.zeros((LANES - 5, LANES), F32)], axis=0
        )
        out_st[at, :] = jnp.transpose(here)

    def whiten_part(x, source, target, start, width):
        tile = min(512, width)

        def tile_step(i, _):
            col = pl.multiple_of(start + i * tile, tile)
            for b in range(blocks):
                at = pl.ds(b * LANES, LANES)
                stats = out_st[at, :]
                position = (col + lax.broadcasted_iota(jnp.int32, (LANES, tile), 1)).astype(F32)
                arrived = source[b * per_block : (b + 1) * per_block, :, pl.ds(col, tile)]
                moved = jnp.dot(
                    out_ch[b], arrived.reshape(LANES, tile), preferred_element_type=F32
                )
                white = (moved - stats[:, x : x + 1]) * stats[:, x + 2 : x + 3]
                white = jnp.where(position < stats[:, 4:5], white, 0.0)
                target[at, pl.ds(col, tile)] = white.astype(BF16)
            return 0

        lax.fori_loop(0, width // tile, tile_step, 0)

    for copy in own + sent:
        copy.wait()
    whiten_part(0, out_r, white_r, 0, span)
    for part, copies in enumerate(second):
        for copy in copies:
            copy.wait_recv()
        whiten_part(1, out_a, white_a, *cuts[part])
    for copies in second:
        for copy in copies:
            copy.wait_send()


def exchange(n_dp, n_group, rewards, values, lengths, decay_rate, piece_dest, row_perm, minibatch):
    rows, span = rewards.shape
    blocks, block = row_perm.shape
    piece = rows // n_dp
    wide = 256
    vmem = pl.BlockSpec(memory_space=pltpu.VMEM)
    far = pl.BlockSpec(memory_space=pltpu.HBM)
    dma = pltpu.SemaphoreType.DMA
    whole = pltpu.VMEM((rows, span), BF16)
    staged = pltpu.VMEM((n_dp, piece, span), BF16)
    factor = pltpu.VMEM((rows, wide), F32)
    column = pltpu.VMEM((rows, LANES), F32)
    small = pltpu.VMEM((n_dp, 8, LANES), F32)
    one = pltpu.VMEM((8, LANES), F32)
    return pl.pallas_call(
        functools.partial(exchange_kernel, n_dp, n_group),
        out_shape=(jax.ShapeDtypeStruct((rows, span), BF16),) * 2,
        in_specs=[vmem, far, vmem, vmem],
        out_specs=(vmem, vmem),
        scratch_shapes=[
            staged, staged, column, pltpu.VMEM((blocks, LANES, LANES), BF16),
            whole, whole, staged, staged,
            pltpu.VMEM((wide, wide), BF16), factor, factor,
            pltpu.VMEM((rows, LANES), jnp.int32), column, column,
            pltpu.VMEM((4, rows, LANES), F32), column, pltpu.VMEM((LANES, LANES), F32),
            small, small, one, small, one, pltpu.VMEM((n_group, 8, LANES), F32),
            pltpu.VMEM((blocks, 8, LANES), F32),
            dma((4,)), dma((2,)), dma((n_dp,)), dma((n_dp,)), dma((3, n_dp)), dma((3, n_dp)),
            dma((n_dp,)), dma((n_dp,)), dma((n_dp,)), dma((n_dp,)), dma((n_group,)), dma((n_group,)),
        ],
        compiler_params=pltpu.CompilerParams(
            collective_id=0, has_side_effects=True, vmem_limit_bytes=50_000_000
        ),
    )(
        rewards, values, decay_rate.reshape(blocks, block),
        jnp.concatenate(
            [
                lengths.reshape(blocks, block),
                row_perm,
                minibatch.reshape(blocks, block),
                jnp.pad(piece_dest, ((0, 0), (0, block - piece_dest.shape[1]))),
            ],
            axis=0,
        ),
    )


def local(n_dp, n_group, rewards, values, lengths, decay_rate, piece_dest, row_perm, minibatch):
    rows, span = rewards.shape
    if (rows // n_dp) % 16 or LANES % (rows // n_dp) or row_perm.shape[1] != LANES or span % 4096:
        return plain_local(rewards, values, lengths, decay_rate, piece_dest, row_perm, minibatch)
    return exchange(
        n_dp, n_group, rewards, values, lengths, decay_rate, piece_dest, row_perm, minibatch
    )


def solution(mesh):
    return jax.shard_map(
        functools.partial(local, mesh.shape["dp"], mesh.shape["group"]),
        mesh=mesh,
        in_specs=(
            P(("dp", "group"), None),
            P(("dp", "group"), None),
            P(("dp", "group")),
            P(("dp", "group")),
            P("dp", None),
            P(("dp", "group"), None),
            P(("dp", "group")),
        ),
        out_specs=(P(("dp", "group"), None), P(("dp", "group"), None)),
        check_vma=False,
    )
```
